32 devices in a mesh: row: 4 (over y, x), col: 8 (over z, core).
Axes of the slice: x: 2, y: 2, z: 4, core: 2. Of those that a mesh axis runs over, the one named last changes fastest.
Arguments:
- mlp_param: float32 [6144, 24576], P('row', 'col'), may hold values from -250 to 250
- mlp_grad: bfloat16 [6144, 24576], P('row', 'col'), may hold values from -250 to 250
- mlp_row_state: float32 [6144], P('row'), may hold values from 0.03 to 2.7
- mlp_col_state: float32 [24576], P('col'), may hold values from 0.02 to 0.3
- attn_param: float32 [6144, 6144], P('row', 'col'), may hold values from -250 to 250
- attn_grad: bfloat16 [6144, 6144], P('row', 'col'), may hold values from -250 to 250
- attn_row_state: float32 [6144], P('row'), may hold values from 0.03 to 2.7
- attn_col_state: float32 [6144], P('col'), may hold values from 0.02 to 0.3
Outputs:
- mlp_param_new: float32 [6144, 24576], P('row', 'col')
- attn_param_new: float32 [6144, 6144], P('row', 'col')
- mlp_row_new: float32 [6144], P('row')
- mlp_col_new: float32 [24576], P('col')
- attn_row_new: float32 [6144], P('row')
- attn_col_new: float32 [6144], P('col')
- attn_copy: bfloat16 [6144, 6144], P(None, 'col')
The draws below stay inside these ranges and needn't reach their ends.
All inputs are finite; a program needn't handle non-finite values.
Results may differ from the reference program's by a relative error of at most 0.0004.
Values may be sent and summed in bfloat16 or wider, within the bound.
A program may use at most 128 MiB of HBM per device.

```python
import math
import jax
import jax.numpy as jnp
from jax import lax

D = 6144
FF = 24576
STEP = 4


def scaled_field(key, height, width, level):
    keys = jax.random.split(key, 3)
    base = jnp.clip(jax.random.normal(keys[0], (height, width), jnp.float32), -4.0, 4.0)
    overall = 1.0
    row_place = jnp.arange(height, dtype=jnp.float32) / height - 0.5
    col_place = jnp.arange(width, dtype=jnp.float32) / width - 0.5
    row_scale = jnp.exp(jax.random.uniform(keys[1], (height,), jnp.float32, -1.15, 1.15)) * jnp.power(3.0, row_place)
    col_scale = jnp.exp(jax.random.uniform(keys[2], (width,), jnp.float32, -1.15, 1.15)) * jnp.power(3.0, col_place)
    row_scale = row_scale / jnp.sqrt(jnp.mean(jnp.square(row_scale)))
    col_scale = col_scale / jnp.sqrt(jnp.mean(jnp.square(col_scale)))
    return level * overall * base * row_scale[:, None] * col_scale[None, :]


def falling_state(key, length):
    jitter = jax.random.uniform(key, (length,), jnp.float32, -0.69, 0.69)
    place = jnp.arange(length, dtype=jnp.float32) / length - 0.5
    return 0.3 * jnp.exp(jitter) * jnp.power(10.0, -place)


def draw_mlp_param(key, part):
    return scaled_field(jax.random.fold_in(key, 11), D, FF, 1.0)


def draw_mlp_grad(key, part):
    return scaled_field(jax.random.fold_in(key, 12), D, FF, 0.4).astype(jnp.bfloat16)


def draw_attn_param(key, part):
    return scaled_field(jax.random.fold_in(key, 13), D, D, 1.0)


def draw_attn_grad(key, part):
    return scaled_field(jax.random.fold_in(key, 14), D, D, 0.4).astype(jnp.bfloat16)


def draw_mlp_row_state(key, part):
    return falling_state(jax.random.fold_in(key, 21), D)


def draw_attn_row_state(key, part):
    return falling_state(jax.random.fold_in(key, 22), D)


def shard_levels(rng, extent, cuts, least, high):
    gain = 1.0
    for position, shards_of in cuts:
        steps = jax.random.uniform(jax.random.fold_in(jax.random.fold_in(rng, 6), position), (shards_of,), jnp.float32, least / len(cuts), high / len(cuts))
        gain = gain * jnp.repeat(jnp.exp(steps), extent[position] // shards_of).reshape((-1,) + (1,) * (len(extent) - 1 - position))
    return gain


def setup_inputs(seed: int = 0) -> dict:
    key_list = jax.random.split(jax.random.key(seed), 9)
    return {
        "mlp_param": draw_mlp_param(jax.random.fold_in(key_list[8], 71), 0),
        "mlp_grad": draw_mlp_grad(jax.random.fold_in(key_list[8], 71), 0),
        "mlp_row_state": draw_mlp_row_state(jax.random.fold_in(key_list[8], 71), 0),
        "mlp_col_state": jnp.clip(jnp.exp(math.log(0.3) - 2.7080503 * jax.random.uniform(key_list[3], (FF,), jnp.float32) ** shard_levels(key_list[3], (FF,), ((0, 8),), -0.2, 0.2)), 0.02, 0.3),
        "attn_param": draw_attn_param(jax.random.fold_in(key_list[8], 71), 0),
        "attn_grad": draw_attn_grad(jax.random.fold_in(key_list[8], 71), 0),
        "attn_row_state": draw_attn_row_state(jax.random.fold_in(key_list[8], 71), 0),
        "attn_col_state": jnp.clip(jnp.exp(math.log(0.3) - 2.7080503 * jax.random.uniform(key_list[7], (D,), jnp.float32) ** shard_levels(key_list[7], (D,), ((0, 8),), -0.2, 0.2)), 0.02, 0.3),
    }


TINY_SQUARE = 1e-30
LEARN_RATE = 0.05
DECAY_POWER = 0.8

def moments(grad, row_state, col_state):
    keep_rate = 1.0 - STEP ** (-DECAY_POWER)
    square = jnp.square(grad.astype(jnp.float32)) + TINY_SQUARE
    rows_new = keep_rate * row_state + (1.0 - keep_rate) * lax.optimization_barrier(jnp.mean(square, axis=1))
    cols_new = keep_rate * col_state + (1.0 - keep_rate) * lax.optimization_barrier(jnp.mean(square, axis=0))
    return (rows_new, cols_new)

def update_matrix(param, grad, rows_new, cols_new):
    raw = grad.astype(jnp.float32) / jnp.sqrt(rows_new[:, None] * cols_new[None, :])
    clip = jnp.maximum(1.0, jnp.sqrt(jnp.mean(jnp.square(raw))))
    step_size = LEARN_RATE * jnp.sqrt(jnp.mean(jnp.square(param)))
    return param - step_size * (raw / clip)

def reference(mlp_param, mlp_grad, mlp_row_state, mlp_col_state, attn_param, attn_grad, attn_row_state, attn_col_state):
    mlp_rows, mlp_cols = moments(mlp_grad, mlp_row_state, mlp_col_state)
    attn_rows, attn_cols = moments(attn_grad, attn_row_state, attn_col_state)
    mlp_new = update_matrix(mlp_param, mlp_grad, mlp_rows, mlp_cols)
    attn_new = update_matrix(attn_param, attn_grad, attn_rows, attn_cols)
    return (mlp_new, attn_new, mlp_rows, mlp_cols, attn_rows, attn_cols, attn_new.astype(jnp.bfloat16))
```

```python
import functools

import jax
import jax.numpy as jnp
from jax import lax
from jax.experimental import pallas as pl
from jax.experimental.pallas import tpu as pltpu
from jax.sharding import PartitionSpec as P

STEP = 4


TINY_SQUARE = 1e-30
LEARN_RATE = 0.05
DECAY_POWER = 0.8


def local(
    mlp_param,
    mlp_grad,
    mlp_row_state,
    mlp_col_state,
    attn_param,
    attn_grad,
    attn_row_state,
    attn_col_state,
):
    keep_rate = 1.0 - STEP ** (-DECAY_POWER)
    block_rows = mlp_grad.shape[0]
    rows_total = block_rows * lax.axis_size("row")
    mlp_width = mlp_grad.shape[1] * lax.axis_size("col")
    attn_width = attn_grad.shape[1] * lax.axis_size("col")
    mlp_count = float(rows_total * mlp_width)
    attn_count = float(rows_total * attn_width)
    mlp_square = jnp.square(mlp_grad.astype(jnp.float32)) + TINY_SQUARE
    attn_square = jnp.square(attn_grad.astype(jnp.float32)) + TINY_SQUARE
    param_local = (jnp.sum(jnp.square(mlp_param)), jnp.sum(jnp.square(attn_param)))
    param_mlp, param_attn = lax.psum((param_local[0], param_local[1]), ("row", "col"))
    row_mlp, row_attn = lax.psum((jnp.sum(mlp_square, axis=1), jnp.sum(attn_square, axis=1)), "col")
    mlp_rows_new = keep_rate * mlp_row_state + (1.0 - keep_rate) * (row_mlp / mlp_width)
    attn_rows_new = keep_rate * attn_row_state + (1.0 - keep_rate) * (row_attn / attn_width)
    col_mlp, col_attn = lax.psum((jnp.sum(mlp_square, axis=0), jnp.sum(attn_square, axis=0)), "row")
    mlp_cols_new = keep_rate * mlp_col_state + (1.0 - keep_rate) * (col_mlp / rows_total)
    attn_cols_new = keep_rate * attn_col_state + (1.0 - keep_rate) * (col_attn / rows_total)
    mlp_raw = mlp_grad.astype(jnp.float32) / jnp.sqrt(mlp_rows_new[:, None] * mlp_cols_new[None, :])
    attn_raw = attn_grad.astype(jnp.float32) / jnp.sqrt(
        attn_rows_new[:, None] * attn_cols_new[None, :]
    )
    clip_local = (jnp.sum(jnp.square(mlp_raw)), jnp.sum(jnp.square(attn_raw)))
    clip_mlp, clip_attn = lax.psum((clip_local[0], clip_local[1]), ("row", "col"))
    mlp_clip = jnp.maximum(1.0, jnp.sqrt(clip_mlp / mlp_count))
    attn_clip = jnp.maximum(1.0, jnp.sqrt(clip_attn / attn_count))
    mlp_step = LEARN_RATE * jnp.sqrt(param_mlp / mlp_count)
    attn_step = LEARN_RATE * jnp.sqrt(param_attn / attn_count)
    mlp_new = mlp_param - mlp_step * (mlp_raw / mlp_clip)
    attn_new = attn_param - attn_step * (attn_raw / attn_clip)
    weight_copy = lax.all_gather(attn_new.astype(jnp.bfloat16), "row", axis=0, tiled=True)
    return (
        mlp_new,
        attn_new,
        mlp_rows_new,
        mlp_cols_new,
        attn_rows_new,
        attn_cols_new,
        weight_copy,
    )


LANES = 128
MESH = pl.DeviceIdType.MESH


def exchange(slots, axis, sems):
    count = slots.shape[0]
    me = lax.axis_index(axis)
    copies = []
    for step in range(1, count):
        copy = pltpu.make_async_remote_copy(
            src_ref=slots.at[me],
            dst_ref=slots.at[me],
            send_sem=sems.at[0, step],
            recv_sem=sems.at[1, step],
            device_id={axis: lax.rem(me + step, count)},
            device_id_type=MESH,
        )
        copy.start()
        copies.append(copy)
    return copies


def finish(copies):
    for copy in copies:
        copy.wait()


def total(slots):
    result = slots[0]
    for rank in range(1, slots.shape[0]):
        result = result + slots[rank]
    return result


def across(row):
    return jnp.transpose(jnp.broadcast_to(row, (LANES, LANES)))


def fold(block):
    result = block[:, :LANES]
    for start in range(LANES, block.shape[1], LANES):
        result = result + block[:, start : start + LANES]
    return result


class Matrix:
    def __init__(self, grad_hbm, param_hbm, row_state, col_state, rows_new, cols_new, scratch):
        self.grad_hbm, self.param_hbm = grad_hbm, param_hbm
        self.row_state, self.col_state = row_state, col_state
        self.rows_new, self.cols_new = rows_new, cols_new
        self.grad, self.param, self.row_slots, self.col_slots, self.near_slots = scratch[:5]
        self.load_sems, self.row_sems, self.col_sems, self.near_sems = scratch[5:]
        self.chunks, self.width = rows_new.shape[0], cols_new.shape[1]

    def load(self, place):
        source, target = ((self.grad_hbm, self.grad), (self.param_hbm, self.param))[place]
        height = self.chunks * LANES // LOADS
        loads = []
        for part in range(LOADS):
            area = pl.ds(part * height, height)
            load = pltpu.make_async_copy(source.at[area], target.at[area], self.load_sems.at[place, part])
            load.start()
            loads.append(load)
        return loads

    def sweep(self, loads, body, carry):
        for part, load in enumerate(loads):
            load.wait()
            carry = lax.fori_loop(
                part * self.chunks // LOADS, (part + 1) * self.chunks // LOADS, body, carry
            )
        return carry

    def first(self, loads):
        me_row, me_col = lax.axis_index("row"), lax.axis_index("col")

        def body(k, cols):
            square = jnp.square(self.grad[rows_of(k), :].astype(jnp.float32)) + TINY_SQUARE
            sums = jnp.sum(jnp.transpose(fold(square)), axis=0, keepdims=True)
            self.row_slots[me_col, pl.ds(k, 1), :] = sums
            return cols + jnp.sum(square.reshape(LANES // 8, 8, self.width), axis=0)

        cols = self.sweep(loads, body, jnp.zeros((8, self.width), jnp.float32))
        self.col_slots[me_row] = jnp.sum(cols, axis=0, keepdims=True)

    def send(self):
        return exchange(self.row_slots, "col", self.row_sems) + exchange(
            self.col_slots, "row", self.col_sems
        )

    def powers(self, loads):
        def body(k, acc):
            square = fold(jnp.square(self.param[rows_of(k), :]))
            return acc + jnp.sum(square.reshape(LANES // 8, 8, LANES), axis=0)

        return self.sweep(loads, body, jnp.zeros((8, LANES), jnp.float32))

    def factors(self):
        keep_rate = 1.0 - STEP ** (-DECAY_POWER)
        width_total = self.width * self.row_slots.shape[0]
        rows_total = self.chunks * LANES * self.col_slots.shape[0]
        rows, cols = total(self.row_slots) / width_total, total(self.col_slots) / rows_total
        self.rows_new[...] = keep_rate * self.row_state[...] + (1.0 - keep_rate) * rows
        self.cols_new[...] = keep_rate * self.col_state[...] + (1.0 - keep_rate) * cols

    def raws(self):
        col_inverse = 1.0 / self.cols_new[...]

        def body(k, acc):
            square = jnp.square(self.grad[rows_of(k), :].astype(jnp.float32))
            part = fold(square * col_inverse) * across(1.0 / self.rows_new[pl.ds(k, 1), :])
            return acc + jnp.sum(part.reshape(LANES // 8, 8, LANES), axis=0)

        return lax.fori_loop(0, self.chunks, body, jnp.zeros((8, LANES), jnp.float32))

    def near(self, raws, powers):
        self.near_slots[lax.axis_index("col")] = jnp.concatenate(
            [jnp.broadcast_to(jnp.sum(v, axis=0, keepdims=True), (4, LANES)) for v in (raws, powers)],
            axis=0,
        )
        return exchange(self.near_slots, "col", self.near_sems)


def rows_of(k):
    return pl.ds(pl.multiple_of(k * LANES, LANES), LANES)


def greet(axes):
    barrier = pltpu.get_barrier_semaphore()
    answers = 0
    for axis, size in axes:
        me = lax.axis_index(axis)
        for step in range(1, size):
            peer = {axis: lax.rem(me + step, size)}
            pl.semaphore_signal(barrier, inc=1, device_id=peer, device_id_type=MESH)
        answers += size - 1
    return answers


def factor_of(far_slots, count):
    sums = jnp.sum(total(far_slots), axis=1, keepdims=True)
    clip = jnp.maximum(1.0, jnp.sqrt(sums[0:1] / count))
    step_size = LEARN_RATE * jnp.sqrt(sums[4:5] / count)
    return jnp.broadcast_to(step_size / clip, (1, LANES))


def stats_kernel(attn_count, mlp_count, *refs):
    ins, outs, scratch = refs[:8], refs[8:16], refs[16:]
    attn = Matrix(*ins[:4], *outs[:2], scratch[:9])
    mlp = Matrix(*ins[4:], *outs[2:4], scratch[9:18])
    coef, low, high, mlp_coef = outs[4:]
    far_slots, far_sems, mlp_far_slots, mlp_far_sems = scratch[18:]
    me_row = lax.axis_index("row")
    ncol, nrow = attn.row_slots.shape[0], attn.col_slots.shape[0]

    attn_grads = attn.load(0)
    attn_params = attn.load(1)
    answers = greet((("col", ncol), ("row", nrow)))
    mlp_grads = mlp.load(0)
    attn.first(attn_grads)
    pl.semaphore_wait(pltpu.get_barrier_semaphore(), answers)
    attn_sends = attn.send()
    mlp_params = mlp.load(1)
    mlp.first(mlp_grads)
    mlp_sends = mlp.send()
    attn_powers = attn.powers(attn_params)
    finish(attn_sends)
    attn.factors()
    attn_near = attn.near(attn.raws(), attn_powers)
    mlp_powers = mlp.powers(mlp_params)
    finish(attn_near)
    far_slots[me_row] = total(attn.near_slots)
    far = exchange(far_slots, "row", far_sems)
    finish(mlp_sends)
    mlp.factors()
    near = mlp.near(mlp.raws(), mlp_powers)
    finish(far)
    factor = factor_of(far_slots, attn_count)
    coef[...] = factor
    col_root = lax.rsqrt(attn.cols_new[...])
    half_chunks = attn.chunks // 2
    for number, half in enumerate((low, high)):

        def update(k, carry):
            place = number * half_chunks + k
            row_root = across(factor * lax.rsqrt(attn.rows_new[pl.ds(place, 1), :]))
            for start in range(0, attn.width, LANES):
                lanes = pl.ds(start, LANES)
                raw = attn.grad[rows_of(place), lanes].astype(jnp.float32) * row_root
                fresh = attn.param[rows_of(place), lanes] - raw * col_root[:, start : start + LANES]
                half[rows_of(k), lanes] = fresh.astype(jnp.bfloat16)
            return carry

        lax.fori_loop(0, half_chunks, update, 0)
        if number == 0:
            finish(near)
            mlp_far_slots[me_row] = total(mlp.near_slots)
            far = exchange(mlp_far_slots, "row", mlp_far_sems)
    finish(far)
    mlp_coef[...] = factor_of(mlp_far_slots, mlp_count)


LOADS = 2


def stats(attn, mlp, nrow, ncol):
    f32 = jnp.float32
    whole = pl.BlockSpec(memory_space=pltpu.VMEM)
    away = pl.BlockSpec(memory_space=pltpu.HBM)
    dma = pltpu.SemaphoreType.DMA
    operands, shapes, scratch = [], [], []
    for param, grad, row_state, col_state in (attn, mlp):
        rows, width = grad.shape
        chunks = rows // LANES
        operands += [grad, param, row_state.reshape(chunks, LANES), col_state.reshape(1, width)]
        shapes += [jax.ShapeDtypeStruct((chunks, LANES), f32), jax.ShapeDtypeStruct((1, width), f32)]
        scratch += [
            pltpu.VMEM((rows, width), grad.dtype),
            pltpu.VMEM((rows, width), f32),
            pltpu.VMEM((ncol, chunks, LANES), f32),
            pltpu.VMEM((nrow, 1, width), f32),
            pltpu.VMEM((ncol, 8, LANES), f32),
            dma((2, LOADS)),
            dma((2, ncol)),
            dma((2, nrow)),
            dma((2, ncol)),
        ]
    rows, width = attn[1].shape
    shapes += [jax.ShapeDtypeStruct((1, LANES), f32)]
    shapes += [jax.ShapeDtypeStruct((rows // 2, width), jnp.bfloat16)] * 2
    shapes += [jax.ShapeDtypeStruct((1, LANES), f32)]
    scratch += [pltpu.VMEM((nrow, 8, LANES), f32), dma((2, nrow))] * 2
    counts = [float(m[1].size * nrow * ncol) for m in (attn, mlp)]
    return pl.pallas_call(
        functools.partial(stats_kernel, *counts),
        out_shape=shapes,
        in_specs=[away, away, whole, whole] * 2,
        out_specs=[whole] * len(shapes),
        scratch_shapes=scratch,
        compiler_params=pltpu.CompilerParams(
            collective_id=0, has_side_effects=True, vmem_limit_bytes=VMEM_BYTES
        ),
        cost_estimate=pl.CostEstimate(
            flops=8 * mlp[1].size, bytes_accessed=8 * mlp[1].size, transcendentals=0
        ),
    )(*operands)


VMEM_BYTES = 66_900_000
PARTS = 4


def place_kernel(picks, masks, extra, *refs):
    count = len(masks)
    pieces, held, sems = refs[:count], refs[-2], refs[-1]
    out, copies = refs[-3 - extra], refs[len(refs) - 2 - extra : -2]
    originals = refs[len(refs) - 3 - 2 * extra : len(refs) - 3 - extra]
    me = lax.axis_index("row")
    rows = held.shape[1]
    size = rows // PARTS
    parts = [(i, part) for i in range(count) for part in range(PARTS)]
    loads = []
    for i, part in parts:
        area = pl.ds(part * size, size)
        load = pltpu.make_async_copy(pieces[i].at[area], held.at[i, area], sems.at[0, i, part])
        load.start()
        loads.append(load)
    for original, duplicate in zip(originals, copies):
        duplicate[...] = original[...]
    stores = []
    for (i, part), load in zip(parts, loads):
        bit_x, bit_y = lax.rem(me, 2), lax.div(me, 2)
        if masks[i] & 1:
            bit_x = 1 - bit_x
        if masks[i] & 2:
            bit_y = 1 - bit_y
        start = ((bit_y * 2 + bit_x) * 2 + picks[i]) * rows + part * size
        load.wait()
        store = pltpu.make_async_copy(
            held.at[i, pl.ds(part * size, size)],
            out.at[pl.ds(pl.multiple_of(start, size), size)],
            sems.at[1, i, part],
        )
        store.start()
        stores.append(store)
    for store in stores:
        store.wait()


def place(pieces, picks, masks, base, vectors):
    rows, width = pieces[0].shape
    count = len(pieces)
    away = pl.BlockSpec(memory_space=pl.ANY)
    whole = pl.BlockSpec(memory_space=pltpu.VMEM)
    operands = list(pieces) + ([] if base is None else [base])
    return pl.pallas_call(
        functools.partial(place_kernel, picks, masks, len(vectors)),
        out_shape=[jax.ShapeDtypeStruct((8 * rows, width), pieces[0].dtype)]
        + [jax.ShapeDtypeStruct(v.shape, v.dtype) for v in vectors],
        in_specs=[away] * len(operands) + [whole] * len(vectors),
        out_specs=[away] + [whole] * len(vectors),
        input_output_aliases={} if base is None else {count: 0},
        scratch_shapes=[
            pltpu.VMEM((count, rows, width), pieces[0].dtype),
            pltpu.SemaphoreType.DMA((2, count, PARTS)),
        ],
        cost_estimate=pl.CostEstimate(
            flops=0, bytes_accessed=4 * count * rows * width, transcendentals=0
        ),
    )(*operands, *vectors)


def root_of(rows_new, coef):
    return coef[0, 0] * lax.rsqrt(rows_new.reshape(-1))


def updated(param, grad, row_root, cols_new):
    return param - (grad.astype(jnp.float32) * row_root[:, None]) * lax.rsqrt(cols_new.reshape(-1))[None, :]


def local_fast(
    nrow,
    ncol,
    mlp_param,
    mlp_grad,
    mlp_row_state,
    mlp_col_state,
    attn_param,
    attn_grad,
    attn_row_state,
    attn_col_state,
):
    attn_rows, attn_cols, mlp_rows, mlp_cols, attn_coef, low, high, mlp_coef = stats(
        (attn_param, attn_grad, attn_row_state, attn_col_state),
        (mlp_param, mlp_grad, mlp_row_state, mlp_col_state),
        nrow,
        ncol,
    )
    over_x = [(i, i ^ 1) for i in range(4)]
    over_y = [(i, i ^ 2) for i in range(4)]
    x_high = lax.ppermute(high, "row", over_x)
    y_low = lax.ppermute(low, "row", over_y)
    mlp_root, low_late, high_late = lax.optimization_barrier((root_of(mlp_rows, mlp_coef), low, high))
    x_low = lax.ppermute(low_late, "row", over_x)
    y_high = lax.ppermute(high_late, "row", over_y)
    mlp_new = updated(mlp_param, mlp_grad, mlp_root, mlp_cols)
    mlp_new, x_high, y_low = lax.optimization_barrier((mlp_new, x_high, y_low))
    far_low = lax.ppermute(y_low, "row", over_x)
    far_high = lax.ppermute(x_high, "row", over_y)
    factors = (mlp_rows, mlp_cols, attn_rows, attn_cols)
    copy, *factors = place((low, high, x_high, y_low), (0, 1, 1, 0), (0, 0, 1, 2), None, factors)
    mlp_rows, mlp_cols, attn_rows, attn_cols = (v.reshape(-1) for v in factors)
    attn_new = updated(attn_param, attn_grad, root_of(attn_rows, attn_coef), attn_cols)
    (copy,) = place((x_low, y_high), (0, 1), (1, 2), copy, ())
    (copy,) = place((far_low, far_high), (0, 1), (3, 3), copy, ())
    return (mlp_new, attn_new, mlp_rows, mlp_cols, attn_rows, attn_cols, copy)


def solution(mesh):
    nrow, ncol = mesh.shape["row"], mesh.shape["col"]

    def step(*args):
        aligned = all(
            a.shape[0] % (4 * LANES) == 0 and a.shape[1] % LANES == 0 for a in (args[0], args[4])
        )
        if nrow == 4 and ncol > 1 and aligned and 6 * (args[0].size + args[4].size) <= VMEM_BYTES * 3 // 4:
            return local_fast(nrow, ncol, *args)
        return local(*args)

    return jax.shard_map(
        step,
        mesh=mesh,
        in_specs=(
            P("row", "col"),
            P("row", "col"),
            P("row"),
            P("col"),
            P("row", "col"),
            P("row", "col"),
            P("row"),
            P("col"),
        ),
        out_specs=(
            P("row", "col"),
            P("row", "col"),
            P("row"),
            P("col"),
            P("row"),
            P("col"),
            P(None, "col"),
        ),
        check_vma=False,
    )
```
